32 devices in a mesh: row: 4 (over y, x), col: 8 (over z, core).
Axes of the slice: x: 2, y: 2, z: 4, core: 2. Of those that a mesh axis runs over, the one named last changes fastest.
Arguments:
- model_gradient: float32 [3, 512, 512, 256], P(None, 'row', 'col'), may hold values from -6 to 6
- filter_x: float32 [512, 512], replicated, may hold values from 0 to 1, as said below
- filter_y: float32 [512, 512], replicated, may hold values from 0 to 1, as said below
- filter_z: float32 [256, 256], replicated, may hold values from 0 to 1, as said below
- depth_scale: float32 [3, 256], replicated, may hold values from 0.3 to 3
Outputs:
- smoothed: float32 [3, 512, 512, 256], P(None, 'row', 'col')
The draws below stay inside these ranges and needn't reach their ends.
Inputs may be any that keep to these rules, and one draw needn't show every extreme that they name: `filter_x`: each row is a nonnegative smoothing kernel of its own width plus one half on the diagonal; rows sum to one. `filter_y`: each row is a nonnegative smoothing kernel of its own width plus one half on the diagonal; rows sum to one. `filter_z`: each row is a nonnegative smoothing kernel of its own width plus one half on the diagonal; rows sum to one.
All inputs are finite; a program needn't handle non-finite values.
Results may differ from the reference program's by a relative error of at most 0.0001.
Values sent between devices are 32-bit elements; how exact they have to be, the bound alone decides.
A program may use at most 192 MiB of HBM per device.

```python
import math
import jax
import jax.numpy as jnp
from jax import lax

PARAMS = 3
NX = 512
NY = 512
NZ = 256


def smoothing_matrix(key, length):
    key_width = jax.random.fold_in(key, 11)
    key_rough = jax.random.fold_in(key, 12)
    lower, upper = (0.5, 1.5)
    widths = length * jnp.exp(jax.random.uniform(key_width, (length, 1), jnp.float32, jnp.log(1.0 / 16.0), jnp.log(1.0 / 4.0)))
    places = jnp.arange(length, dtype=jnp.float32)
    apart = places[:, None] - places[None, :]
    rough = jax.random.uniform(key_rough, (length, length), jnp.float32, lower, upper)
    kernel = jnp.exp(-apart * apart / (2.0 * widths * widths)) * rough
    kernel = 0.5 * kernel / jnp.sum(kernel, axis=1, keepdims=True)
    return kernel + 0.5 * jnp.eye(length, dtype=jnp.float32)


def draw_filter_x(key, part):
    return smoothing_matrix(jax.random.fold_in(key, 1), NX)


def draw_filter_y(key, part):
    return smoothing_matrix(jax.random.fold_in(key, 2), NY)


def draw_filter_z(key, part):
    return smoothing_matrix(jax.random.fold_in(key, 3), NZ)


def steps_of(rng, dims, pieces, smallest, high):
    factor_of = 1.0
    for position, blocks in pieces:
        heights = jax.random.uniform(jax.random.fold_in(jax.random.fold_in(rng, 6), position), (blocks,), jnp.float32, smallest / len(pieces), high / len(pieces))
        factor_of = factor_of * jnp.repeat(jnp.exp(heights), dims[position] // blocks).reshape((-1,) + (1,) * (len(dims) - 1 - position))
    return factor_of


def normal_values(key, dims, deviation, limit, cuts=(), held_as=jnp.bfloat16):
    gain = steps_of(key, dims, cuts, -0.22, 0.18) if cuts else 1.0
    result = jax.random.normal(key, dims, jnp.float32) * deviation * gain
    return jnp.minimum(jnp.maximum(result, -limit), limit).astype(held_as)


def setup_inputs(seed: int = 0) -> dict:
    keys = jax.random.split(jax.random.key(seed), 6)
    return {
        "model_gradient": normal_values(keys[0], (PARAMS, NX, NY, NZ), 1.0, 6.0, ((1, 4), (2, 8)), jnp.float32),
        "filter_x": draw_filter_x(jax.random.fold_in(keys[5], 71), 0),
        "filter_y": draw_filter_y(jax.random.fold_in(keys[5], 71), 0),
        "filter_z": draw_filter_z(jax.random.fold_in(keys[5], 71), 0),
        "depth_scale": jnp.clip(jnp.exp(jax.random.uniform(keys[4], (PARAMS, NZ), jnp.float32, math.log(0.3), math.log(3.0))), 0.3, 3.0),
    }


def reference(model_gradient, filter_x, filter_y, filter_z, depth_scale):
    highest_accuracy = lax.Precision.HIGHEST
    results = []
    for index in range(PARAMS):
        field = model_gradient[index]
        depth_pass = jnp.einsum("abz,kz->abk", field, filter_z, precision=highest_accuracy)
        depth_pass = depth_pass * depth_scale[index][None, None, :]
        initial_sweep = jnp.einsum("ia,abk->ibk", filter_x, depth_pass, precision=highest_accuracy)
        second_pass = jnp.einsum("jb,ibk->ijk", filter_y, initial_sweep, precision=highest_accuracy)
        results.append(second_pass)
    return jnp.stack(results)
```

```python
import functools

import jax
import jax.numpy as jnp
from jax import lax
from jax.experimental import pallas as pl
from jax.experimental.pallas import tpu as pltpu
from jax.sharding import PartitionSpec as P

ACCURACY = lax.Precision.HIGH
AXES = ("row", "col")
INNER = (((1,), (0,)), ((), ()))
MESH = pl.DeviceIdType.MESH
LANES, SUBLANES = 128, 8
STAGING_LIMIT = 48 * 2**20
VMEM_LIMIT = 62 * 2**20


def split(value):
    high = value.astype(jnp.bfloat16)
    return high, (value - high.astype(jnp.float32)).astype(jnp.bfloat16)


def dot3(left, right):
    def one(a, b):
        return lax.dot_general(a, b, INNER, preferred_element_type=jnp.float32)

    return one(left[0], right[0]) + (one(left[0], right[1]) + one(left[1], right[0]))


def wait_bytes(ref, sem):
    pltpu.make_async_copy(ref, ref, sem).wait()


def smooth_kernel(
    rows, cols, field, filter_x, filter_y, filter_z, scale, out, home,
    ybuf, xbuf, raw_x, raw_y, raw_z, raw_s, pair_x, pair_y, pair_z,
    load_sem, yf_recv, yb_recv, xf_recv, xb_recv, yf_send, yb_send, xf_send, xb_send,
):
    row, col = lax.axis_index("row"), lax.axis_index("col")
    params, xloc, yloc, depth = field.shape
    ychunks, ca = ybuf.shape[1], ybuf.shape[3]
    xchunks, cb = xbuf.shape[1], xbuf.shape[4]
    xa, yb = xloc // cols, yloc // rows

    loads = [
        pltpu.make_async_copy(given, raw, load_sem.at[n])
        for n, (given, raw) in enumerate(
            [(filter_x, raw_x), (filter_y, raw_y), (filter_z, raw_z), (scale, raw_s)]
        )
    ]
    for load in loads:
        load.start()

    barrier = pltpu.get_barrier_semaphore()

    @pl.loop(1, cols)
    def _(j):
        peer = (row, lax.rem(col + j, cols))
        pl.semaphore_signal(barrier, inc=1, device_id=peer, device_id_type=MESH)

    @pl.loop(1, rows)
    def _(j):
        peer = (lax.rem(row + j, rows), col)
        pl.semaphore_signal(barrier, inc=1, device_id=peer, device_id_type=MESH)

    pl.semaphore_wait(barrier, rows + cols - 2)

    def a_range(part, c):
        return pl.ds(part * xa + c * ca, ca)

    def b_range(part, c):
        return pl.ds(pl.multiple_of(part * yb + c * cb, SUBLANES), cb)

    def send_y(p, source):
        @pl.loop(0, ychunks)
        def _(c):
            pltpu.make_async_copy(
                source.at[p, a_range(col, c)], ybuf.at[p, c, col], yf_recv.at[p, c]
            ).start()

            @pl.loop(1, cols)
            def _(j):
                to = lax.rem(col + j, cols)
                pltpu.make_async_remote_copy(
                    source.at[p, a_range(to, c)],
                    ybuf.at[p, c, col],
                    yf_send.at[p],
                    yf_recv.at[p, c],
                    device_id=(row, to),
                    device_id_type=MESH,
                ).start()

    def return_y(p, c, target):
        pltpu.make_async_copy(
            ybuf.at[p, c, col], target.at[p, a_range(col, c)], yb_recv.at[p]
        ).start()

        @pl.loop(1, cols)
        def _(j):
            to = lax.rem(col + j, cols)
            pltpu.make_async_remote_copy(
                ybuf.at[p, c, to],
                target.at[p, a_range(col, c)],
                yb_send.at[p],
                yb_recv.at[p],
                device_id=(row, to),
                device_id_type=MESH,
            ).start()

    def send_x(p, source):
        @pl.loop(0, xchunks)
        def _(c):
            pltpu.make_async_copy(
                source.at[p, :, b_range(row, c)], xbuf.at[p, c, row], xf_recv.at[p, c]
            ).start()

            @pl.loop(1, rows)
            def _(j):
                to = lax.rem(row + j, rows)
                pltpu.make_async_remote_copy(
                    source.at[p, :, b_range(to, c)],
                    xbuf.at[p, c, row],
                    xf_send.at[p],
                    xf_recv.at[p, c],
                    device_id=(to, col),
                    device_id_type=MESH,
                ).start()

    def return_x(p, c, target):
        pltpu.make_async_copy(
            xbuf.at[p, c, row], target.at[p, :, b_range(row, c)], xb_recv.at[p]
        ).start()

        @pl.loop(1, rows)
        def _(j):
            to = lax.rem(row + j, rows)
            pltpu.make_async_remote_copy(
                xbuf.at[p, c, to],
                target.at[p, :, b_range(row, c)],
                xb_send.at[p],
                xb_recv.at[p],
                device_id=(to, col),
                device_id_type=MESH,
            ).start()

    def prepare():
        for load in loads:
            load.wait()
        for raw, pair in ((raw_x, pair_x), (raw_y, pair_y)):
            pair[0], pair[1] = split(raw[...])
        turned = raw_z[...].T
        for p in range(params):
            pair_z[p, 0], pair_z[p, 1] = split(turned * raw_s[pl.ds(p, 1), :])

    def filter_y_depth(p, c):
        wait_bytes(ybuf.at[p, c], yf_recv.at[p, c])

        @pl.loop(0, ca)
        def _(a):
            plane = ybuf[p, c, :, a].reshape(cols * yloc, depth)
            column = dot3(split(plane), (pair_z[p, 0], pair_z[p, 1]))
            value = dot3((pair_y[0], pair_y[1]), split(column))
            ybuf[p, c, :, a] = value.reshape(cols, yloc, depth)

    def filter_x_rows(p, c):
        wait_bytes(xbuf.at[p, c], xf_recv.at[p, c])
        for b in range(cb):
            plane = xbuf[p, c, :, :, b, :].reshape(rows * xloc, depth)
            value = dot3((pair_x[0], pair_x[1]), split(plane))
            xbuf[p, c, :, :, b, :] = value.reshape(rows, xloc, depth)

    @pl.loop(0, params)
    def _(q):
        x_param = lax.rem(q + 1, params)

        @pl.when(q == 0)
        def _():
            send_y(0, field)
            send_x(1, field)
            prepare()

        @pl.when(q > 0)
        def _():
            wait_bytes(home.at[q], xb_recv.at[q])
            send_y(q, home)

            @pl.when(q < params - 1)
            def _():
                send_x(q + 1, field)

            @pl.when(q == params - 1)
            def _():
                wait_bytes(home.at[0], yb_recv.at[0])
                send_x(0, home)

        @pl.loop(0, max(xchunks, ychunks))
        def _(c):
            @pl.when(c < xchunks)
            def _():
                filter_x_rows(x_param, c)

                @pl.when(x_param > 0)
                def _():
                    return_x(x_param, c, home)

                @pl.when(x_param == 0)
                def _():
                    return_x(0, c, out)

            @pl.when(c < ychunks)
            def _():
                filter_y_depth(q, c)

                @pl.when(q == 0)
                def _():
                    return_y(0, c, home)

                @pl.when(q > 0)
                def _():
                    return_y(q, c, out)

    wait_bytes(out.at[0], xb_recv.at[0])

    @pl.loop(0, params)
    def _(p):
        @pl.when(p > 0)
        def _():
            wait_bytes(out.at[p], yb_recv.at[p])

        for sem in (yf_send, yb_send):
            wait_bytes(home.at[p, pl.ds(0, xloc - xa)], sem.at[p])
        for sem in (xf_send, xb_send):
            wait_bytes(home.at[p, :, pl.ds(0, yloc - yb)], sem.at[p])


def kernel_shards(model_gradient, filter_x, filter_y, filter_z, depth_scale):
    rows, cols = lax.axis_size("row"), lax.axis_size("col")
    params, xloc, yloc, depth = model_gradient.shape
    nx, ny = filter_x.shape[0], filter_y.shape[0]
    ychunks = y_chunks(xloc // cols)
    ca = xloc // cols // ychunks
    cb = SUBLANES
    xchunks = yloc // rows // cb
    whole = pl.BlockSpec(memory_space=pl.ANY)
    full = jax.ShapeDtypeStruct(model_gradient.shape, jnp.float32)
    dma = pltpu.SemaphoreType.DMA
    flops = 6 * model_gradient.size * (nx + ny + depth)
    out, _ = pl.pallas_call(
        functools.partial(smooth_kernel, rows, cols),
        in_specs=[whole] * 5,
        out_specs=[whole, whole],
        out_shape=[full, full],
        scratch_shapes=[
            pltpu.VMEM((params, ychunks, cols, ca, yloc, depth), jnp.float32),
            pltpu.VMEM((params, xchunks, rows, xloc, cb, depth), jnp.float32),
            pltpu.VMEM(filter_x.shape, jnp.float32),
            pltpu.VMEM(filter_y.shape, jnp.float32),
            pltpu.VMEM(filter_z.shape, jnp.float32),
            pltpu.VMEM(depth_scale.shape, jnp.float32),
            pltpu.VMEM((2,) + filter_x.shape, jnp.bfloat16),
            pltpu.VMEM((2,) + filter_y.shape, jnp.bfloat16),
            pltpu.VMEM((params, 2) + filter_z.shape, jnp.bfloat16),
            dma((4,)),
            dma((params, ychunks)),
            dma((params,)),
            dma((params, xchunks)),
            dma((params,)),
            dma((params,)),
            dma((params,)),
            dma((params,)),
            dma((params,)),
        ],
        cost_estimate=pl.CostEstimate(
            flops=flops, bytes_accessed=32 * model_gradient.size, transcendentals=0
        ),
        compiler_params=pltpu.CompilerParams(
            collective_id=0, has_side_effects=True, vmem_limit_bytes=VMEM_LIMIT
        ),
    )(model_gradient, filter_x, filter_y, filter_z, depth_scale)
    return out


def y_chunks(planes):
    return 4 if planes % 4 == 0 else 1


def fits(shape, rows, cols):
    params, xloc, yloc, depth = shape
    aligned = xloc % cols == 0 and yloc % (rows * SUBLANES) == 0 and depth % LANES == 0
    staged = 2 * 4 * params * xloc * yloc * depth
    return aligned and params > 1 and staged <= STAGING_LIMIT


def plane_filter(incoming, filter_x, filter_y, rows, cols):
    xloc, yloc = incoming.shape[0], incoming.shape[1]
    matrix_x = filter_x.reshape(rows, xloc, rows, xloc)
    matrix_y = filter_y.reshape(cols, yloc, cols, yloc)
    partial_value = jnp.einsum(
        "ABRa,abRSz->ABbSz", matrix_x, incoming, precision=ACCURACY
    )
    return jnp.einsum(
        "CDSb,ABbSz->ACBDz", matrix_y, partial_value, precision=ACCURACY
    )


def plain_shards(model_gradient, filter_x, filter_y, filter_z, depth_scale):
    rows, cols = lax.axis_size("row"), lax.axis_size("col")
    params, xloc, yloc, depth = model_gradient.shape
    parts = rows * cols
    block = depth // parts
    arrived = []
    for index in range(params):
        scaled_filter = depth_scale[index][:, None] * filter_z
        column = jnp.einsum(
            "kz,abz->abk", scaled_filter, model_gradient[index], precision=ACCURACY
        )
        outgoing = column.reshape(xloc, yloc, parts, block)
        arrived.append(
            lax.all_to_all(outgoing, AXES, split_axis=2, concat_axis=2, tiled=True)
        )
    results = []
    for index in range(params):
        incoming = arrived[index].reshape(xloc, yloc, rows, cols, block)
        planes = plane_filter(incoming, filter_x, filter_y, rows, cols)
        planes = planes.reshape(parts, xloc, yloc, block)
        back = lax.all_to_all(planes, AXES, split_axis=0, concat_axis=3, tiled=True)
        results.append(back.reshape(xloc, yloc, depth))
    return jnp.stack(results)


def shards(model_gradient, filter_x, filter_y, filter_z, depth_scale):
    rows, cols = lax.axis_size("row"), lax.axis_size("col")
    chosen = kernel_shards if fits(model_gradient.shape, rows, cols) else plain_shards
    return chosen(model_gradient, filter_x, filter_y, filter_z, depth_scale)


def solution(mesh):
    return jax.shard_map(
        shards,
        mesh=mesh,
        in_specs=(P(None, "row", "col", None), P(), P(), P(), P()),
        out_specs=P(None, "row", "col", None),
        check_vma=False,
    )
```

```python
import functools

import jax
import jax.numpy as jnp
from jax import lax
from jax.experimental import pallas as pl
from jax.experimental.pallas import tpu as pltpu
from jax.sharding import PartitionSpec as P

ACCURACY = lax.Precision.HIGH
AXES = ("row", "col")
INNER = (((1,), (0,)), ((), ()))
MESH = pl.DeviceIdType.MESH
LANES, SUBLANES = 128, 8
PLACE_PLANES = 8
SPARE = 2 * 2**20
STAGING_LIMIT = 48 * 2**20
VMEM_LIMIT = 62 * 2**20


def split(value):
    high = value.astype(jnp.bfloat16)
    return high, (value - high.astype(jnp.float32)).astype(jnp.bfloat16)


def dot3(left, right):
    def one(a, b):
        return lax.dot_general(a, b, INNER, preferred_element_type=jnp.float32)

    return one(left[0], right[0]) + (one(left[0], right[1]) + one(left[1], right[0]))


def wait_bytes(ref, sem):
    pltpu.make_async_copy(ref, ref, sem).wait()


def smooth_kernel(
    rows, cols, tail, field, filter_x, filter_y, filter_z, scale, out, home, rest,
    ybuf, xbuf, raw_x, raw_y, raw_z, raw_s, pair_x, pair_y, pair_z,
    load_sem, rest_sem, yf_recv, yb_recv, xf_recv, xb_recv, yf_send, yb_send, xf_send, xb_send,
):
    row, col = lax.axis_index("row"), lax.axis_index("col")
    params, xloc, yloc, depth = field.shape
    ychunks, ca = ybuf.shape[1], ybuf.shape[3]
    xchunks, cb = xbuf.shape[1], xbuf.shape[4]
    xa, yb = xloc // cols, yloc // rows
    last, half = params - 1, cols // 2

    loads = [
        pltpu.make_async_copy(given, raw, load_sem.at[n])
        for n, (given, raw) in enumerate(
            [(filter_x, raw_x), (filter_y, raw_y), (filter_z, raw_z), (scale, raw_s)]
        )
    ]
    for load in loads:
        load.start()

    barrier = pltpu.get_barrier_semaphore()

    @pl.loop(1, cols)
    def _(j):
        peer = (row, lax.rem(col + j, cols))
        pl.semaphore_signal(barrier, inc=1, device_id=peer, device_id_type=MESH)

    @pl.loop(1, rows)
    def _(j):
        peer = (lax.rem(row + j, rows), col)
        pl.semaphore_signal(barrier, inc=1, device_id=peer, device_id_type=MESH)

    pl.semaphore_wait(barrier, rows + cols - 2)

    def a_range(part, c):
        return pl.ds(part * xa + c * ca, ca)

    def b_range(part, c):
        return pl.ds(pl.multiple_of(part * yb + c * cb, SUBLANES), cb)

    def send_y(p, source):
        @pl.loop(0, ychunks)
        def _(c):
            pltpu.make_async_copy(
                source.at[p, a_range(col, c)], ybuf.at[p, c, col], yf_recv.at[p, c]
            ).start()

            @pl.loop(1, cols)
            def _(j):
                to = lax.rem(col + j, cols)
                pltpu.make_async_remote_copy(
                    source.at[p, a_range(to, c)],
                    ybuf.at[p, c, col],
                    yf_send.at[p],
                    yf_recv.at[p, c],
                    device_id=(row, to),
                    device_id_type=MESH,
                ).start()

    def return_y(p, c, target):
        pltpu.make_async_copy(
            ybuf.at[p, c, col], target.at[p, a_range(col, c)], yb_recv.at[p]
        ).start()

        kept = (p == last) & (c >= ychunks - tail)

        @pl.loop(1, cols)
        def _(j):
            to = lax.rem(col + j, cols)

            @pl.when(jnp.logical_not(kept & (j == half)))
            def _():
                pltpu.make_async_remote_copy(
                    ybuf.at[p, c, to],
                    target.at[p, a_range(col, c)],
                    yb_send.at[p],
                    yb_recv.at[p],
                    device_id=(row, to),
                    device_id_type=MESH,
                ).start()

        @pl.when(kept)
        def _():
            pltpu.make_async_copy(
                ybuf.at[p, c, lax.rem(col + half, cols)],
                rest.at[pl.ds((c - (ychunks - tail)) * ca, ca)],
                rest_sem,
            ).start()

    def send_x(p, source):
        @pl.loop(0, xchunks)
        def _(c):
            pltpu.make_async_copy(
                source.at[p, :, b_range(row, c)], xbuf.at[p, c, row], xf_recv.at[p, c]
            ).start()

            @pl.loop(1, rows)
            def _(j):
                to = lax.rem(row + j, rows)
                pltpu.make_async_remote_copy(
                    source.at[p, :, b_range(to, c)],
                    xbuf.at[p, c, row],
                    xf_send.at[p],
                    xf_recv.at[p, c],
                    device_id=(to, col),
                    device_id_type=MESH,
                ).start()

    def return_x(p, c, target):
        pltpu.make_async_copy(
            xbuf.at[p, c, row], target.at[p, :, b_range(row, c)], xb_recv.at[p]
        ).start()

        @pl.loop(1, rows)
        def _(j):
            to = lax.rem(row + j, rows)
            pltpu.make_async_remote_copy(
                xbuf.at[p, c, to],
                target.at[p, :, b_range(row, c)],
                xb_send.at[p],
                xb_recv.at[p],
                device_id=(to, col),
                device_id_type=MESH,
            ).start()

    def prepare():
        for load in loads:
            load.wait()
        for raw, pair in ((raw_x, pair_x), (raw_y, pair_y)):
            pair[0], pair[1] = split(raw[...])
        turned = raw_z[...].T
        for p in range(params):
            pair_z[p, 0], pair_z[p, 1] = split(turned * raw_s[pl.ds(p, 1), :])

    def filter_y_depth(p, c):
        wait_bytes(ybuf.at[p, c], yf_recv.at[p, c])

        @pl.loop(0, ca)
        def _(a):
            plane = ybuf[p, c, :, a].reshape(cols * yloc, depth)
            column = dot3(split(plane), (pair_z[p, 0], pair_z[p, 1]))
            value = dot3((pair_y[0], pair_y[1]), split(column))
            ybuf[p, c, :, a] = value.reshape(cols, yloc, depth)

    def filter_x_rows(p, c):
        wait_bytes(xbuf.at[p, c], xf_recv.at[p, c])
        for b in range(cb):
            plane = xbuf[p, c, :, :, b, :].reshape(rows * xloc, depth)
            value = dot3((pair_x[0], pair_x[1]), split(plane))
            xbuf[p, c, :, :, b, :] = value.reshape(rows, xloc, depth)

    @pl.loop(0, params)
    def _(q):
        x_param = lax.rem(q + 1, params)

        @pl.when(q == 0)
        def _():
            send_y(0, field)
            send_x(1, field)
            prepare()

        @pl.when(q > 0)
        def _():
            wait_bytes(home.at[q], xb_recv.at[q])
            send_y(q, home)

            @pl.when(q < params - 1)
            def _():
                send_x(q + 1, field)

            @pl.when(q == params - 1)
            def _():
                wait_bytes(home.at[0], yb_recv.at[0])
                send_x(0, home)

        @pl.loop(0, max(xchunks, ychunks))
        def _(c):
            @pl.when(c < xchunks)
            def _():
                filter_x_rows(x_param, c)

                @pl.when(x_param > 0)
                def _():
                    return_x(x_param, c, home)

                @pl.when(x_param == 0)
                def _():
                    return_x(0, c, out)

            @pl.when(c < ychunks)
            def _():
                filter_y_depth(q, c)

                @pl.when(q == 0)
                def _():
                    return_y(0, c, home)

                @pl.when(q > 0)
                def _():
                    return_y(q, c, out)

    wait_bytes(out.at[0], xb_recv.at[0])

    @pl.loop(0, params)
    def _(p):
        wait_bytes(home.at[p, pl.ds(0, xloc - xa)], yf_send.at[p])

        @pl.when(p < last)
        def _():
            wait_bytes(home.at[p, pl.ds(0, xloc - xa)], yb_send.at[p])

            @pl.when(p > 0)
            def _():
                wait_bytes(out.at[p], yb_recv.at[p])

        @pl.when(p == last)
        def _():
            sent = xloc - tail * ca
            wait_bytes(out.at[p, pl.ds(0, sent)], yb_recv.at[p])
            wait_bytes(home.at[p, pl.ds(0, sent - xa)], yb_send.at[p])
            wait_bytes(rest, rest_sem)

        for sem in (xf_send, xb_send):
            wait_bytes(home.at[p, :, pl.ds(0, yloc - yb)], sem.at[p])


def place_kernel(given, out, slots, reads, writes):
    count, planes = slots.shape[:2]
    per = given.shape[1] // planes

    def part(ref, n):
        return ref.at[n // per, pl.ds(n % per * planes, planes)]

    def read(n):
        return pltpu.make_async_copy(part(given, n), slots.at[n], reads.at[n])

    def write(n):
        return pltpu.make_async_copy(slots.at[n], part(out, n), writes.at[n])

    for n in range(count):
        read(n).start()
    for n in range(count):
        read(n).wait()
        write(n).start()
    for n in range(count):
        write(n).wait()


def place(field):
    params, xloc, yloc, depth = field.shape
    planes = max(n for n in range(1, PLACE_PLANES + 1) if xloc % n == 0)
    count = params * xloc // planes
    return pl.pallas_call(
        place_kernel,
        in_specs=[pl.BlockSpec(memory_space=pl.ANY)],
        out_specs=pl.BlockSpec(memory_space=pl.ANY),
        out_shape=jax.ShapeDtypeStruct(field.shape, jnp.float32),
        scratch_shapes=[
            pltpu.VMEM((count, planes, yloc, depth), jnp.float32),
            pltpu.SemaphoreType.DMA((count,)),
            pltpu.SemaphoreType.DMA((count,)),
        ],
        cost_estimate=pl.CostEstimate(
            flops=512 * field.size, bytes_accessed=8 * field.size, transcendentals=0
        ),
        compiler_params=pltpu.CompilerParams(vmem_limit_bytes=VMEM_LIMIT - SPARE),
    )(field)


def insert_kernel(cols, landed, _, out, sem):
    params, xloc = out.shape[:2]
    planes, xa = landed.shape[0], xloc // cols
    source = lax.rem(lax.axis_index("col") + cols // 2, cols)
    target = out.at[params - 1, pl.ds((source + 1) * xa - planes, planes)]
    move = pltpu.make_async_copy(landed, target, sem)
    move.start()
    move.wait()


def insert(field, landed, cols):
    return pl.pallas_call(
        functools.partial(insert_kernel, cols),
        in_specs=[pl.BlockSpec(memory_space=pltpu.VMEM), pl.BlockSpec(memory_space=pl.ANY)],
        out_specs=pl.BlockSpec(memory_space=pl.ANY),
        out_shape=jax.ShapeDtypeStruct(field.shape, jnp.float32),
        input_output_aliases={1: 0},
        scratch_shapes=[pltpu.SemaphoreType.DMA],
        cost_estimate=pl.CostEstimate(
            flops=landed.size, bytes_accessed=8 * landed.size, transcendentals=0
        ),
        compiler_params=pltpu.CompilerParams(vmem_limit_bytes=SPARE),
    )(landed, field)


def kernel_shards(model_gradient, filter_x, filter_y, filter_z, depth_scale):
    rows, cols = lax.axis_size("row"), lax.axis_size("col")
    params, xloc, yloc, depth = model_gradient.shape
    nx, ny = filter_x.shape[0], filter_y.shape[0]
    ychunks = y_chunks(xloc // cols)
    ca = xloc // cols // ychunks
    tail = max(1, ychunks // 2)
    cb = SUBLANES
    xchunks = yloc // rows // cb
    whole = pl.BlockSpec(memory_space=pl.ANY)
    full = jax.ShapeDtypeStruct(model_gradient.shape, jnp.float32)
    dma = pltpu.SemaphoreType.DMA
    flops = 6 * model_gradient.size * (nx + ny + depth)
    held = jax.ShapeDtypeStruct((tail * ca, yloc, depth), jnp.float32)
    out, _, rest = pl.pallas_call(
        functools.partial(smooth_kernel, rows, cols, tail),
        in_specs=[whole] * 5,
        out_specs=[whole] * 3,
        out_shape=[full, full, held],
        scratch_shapes=[
            pltpu.VMEM((params, ychunks, cols, ca, yloc, depth), jnp.float32),
            pltpu.VMEM((params, xchunks, rows, xloc, cb, depth), jnp.float32),
            pltpu.VMEM(filter_x.shape, jnp.float32),
            pltpu.VMEM(filter_y.shape, jnp.float32),
            pltpu.VMEM(filter_z.shape, jnp.float32),
            pltpu.VMEM(depth_scale.shape, jnp.float32),
            pltpu.VMEM((2,) + filter_x.shape, jnp.bfloat16),
            pltpu.VMEM((2,) + filter_y.shape, jnp.bfloat16),
            pltpu.VMEM((params, 2) + filter_z.shape, jnp.bfloat16),
            dma((4,)),
            dma,
            dma((params, ychunks)),
            dma((params,)),
            dma((params, xchunks)),
            dma((params,)),
            dma((params,)),
            dma((params,)),
            dma((params,)),
            dma((params,)),
        ],
        cost_estimate=pl.CostEstimate(
            flops=flops, bytes_accessed=32 * model_gradient.size, transcendentals=0
        ),
        compiler_params=pltpu.CompilerParams(
            collective_id=0, has_side_effects=True, vmem_limit_bytes=VMEM_LIMIT
        ),
    )(model_gradient, filter_x, filter_y, filter_z, depth_scale)
    swap = [(s, (s + cols // 2) % cols) for s in range(cols)]
    landed = lax.ppermute(rest, "col", swap)
    return insert(place(out), landed, cols)


def y_chunks(planes):
    return 4 if planes % 4 == 0 else 1


def fits(shape, rows, cols):
    params, xloc, yloc, depth = shape
    aligned = cols % 2 == 0 and xloc % cols == 0 and depth % LANES == 0
    aligned = aligned and yloc % (rows * SUBLANES) == 0
    staged = 2 * 4 * params * xloc * yloc * depth
    return aligned and params > 1 and staged <= STAGING_LIMIT


def plane_filter(incoming, filter_x, filter_y, rows, cols):
    xloc, yloc = incoming.shape[0], incoming.shape[1]
    matrix_x = filter_x.reshape(rows, xloc, rows, xloc)
    matrix_y = filter_y.reshape(cols, yloc, cols, yloc)
    partial_value = jnp.einsum(
        "ABRa,abRSz->ABbSz", matrix_x, incoming, precision=ACCURACY
    )
    return jnp.einsum(
        "CDSb,ABbSz->ACBDz", matrix_y, partial_value, precision=ACCURACY
    )


def plain_shards(model_gradient, filter_x, filter_y, filter_z, depth_scale):
    rows, cols = lax.axis_size("row"), lax.axis_size("col")
    params, xloc, yloc, depth = model_gradient.shape
    parts = rows * cols
    block = depth // parts
    arrived = []
    for index in range(params):
        scaled_filter = depth_scale[index][:, None] * filter_z
        column = jnp.einsum(
            "kz,abz->abk", scaled_filter, model_gradient[index], precision=ACCURACY
        )
        outgoing = column.reshape(xloc, yloc, parts, block)
        arrived.append(
            lax.all_to_all(outgoing, AXES, split_axis=2, concat_axis=2, tiled=True)
        )
    results = []
    for index in range(params):
        incoming = arrived[index].reshape(xloc, yloc, rows, cols, block)
        planes = plane_filter(incoming, filter_x, filter_y, rows, cols)
        planes = planes.reshape(parts, xloc, yloc, block)
        back = lax.all_to_all(planes, AXES, split_axis=0, concat_axis=3, tiled=True)
        results.append(back.reshape(xloc, yloc, depth))
    return jnp.stack(results)


def shards(model_gradient, filter_x, filter_y, filter_z, depth_scale):
    rows, cols = lax.axis_size("row"), lax.axis_size("col")
    chosen = kernel_shards if fits(model_gradient.shape, rows, cols) else plain_shards
    return chosen(model_gradient, filter_x, filter_y, filter_z, depth_scale)


def solution(mesh):
    return jax.shard_map(
        shards,
        mesh=mesh,
        in_specs=(P(None, "row", "col", None), P(), P(), P(), P()),
        out_specs=P(None, "row", "col", None),
        check_vma=False,
    )
```

```python
import functools

import jax
import jax.numpy as jnp
from jax import lax
from jax.experimental import pallas as pl
from jax.experimental.pallas import tpu as pltpu
from jax.sharding import PartitionSpec as P

ACCURACY = lax.Precision.HIGH
AXES = ("row", "col")
INNER = (((1,), (0,)), ((), ()))
MESH = pl.DeviceIdType.MESH
LANES, SUBLANES = 128, 8
PLACE_PLANES = 8
SPARE = 2 * 2**20
STAGING_LIMIT = 48 * 2**20
VMEM_LIMIT = 62 * 2**20


def split(value):
    high = value.astype(jnp.bfloat16)
    return high, (value - high.astype(jnp.float32)).astype(jnp.bfloat16)


def dot3(left, right):
    def one(a, b):
        return lax.dot_general(a, b, INNER, preferred_element_type=jnp.float32)

    return one(left[0], right[0]) + (one(left[0], right[1]) + one(left[1], right[0]))


def wait_bytes(ref, sem):
    pltpu.make_async_copy(ref, ref, sem).wait()


def smooth_kernel(
    rows, cols, tail, field, filter_x, filter_y, filter_z, scale, out, home, rest,
    ybuf, xbuf, raw_x, raw_y, raw_z, raw_s, pair_x, pair_y, pair_z,
    load_sem, rest_sem, yf_recv, yb_recv, xf_recv, xb_recv, yf_send, yb_send, xf_send, xb_send,
):
    row, col = lax.axis_index("row"), lax.axis_index("col")
    params, xloc, yloc, depth = field.shape
    ychunks, ca = ybuf.shape[1], ybuf.shape[3]
    xchunks, cb = xbuf.shape[1], xbuf.shape[4]
    xa, yb = xloc // cols, yloc // rows
    last, half = params - 1, cols // 2

    loads = [
        pltpu.make_async_copy(given, raw, load_sem.at[n])
        for n, (given, raw) in enumerate(
            [(filter_x, raw_x), (filter_y, raw_y), (filter_z, raw_z), (scale, raw_s)]
        )
    ]
    for load in loads:
        load.start()

    barrier = pltpu.get_barrier_semaphore()

    @pl.loop(1, cols)
    def _(j):
        peer = (row, lax.rem(col + j, cols))
        pl.semaphore_signal(barrier, inc=1, device_id=peer, device_id_type=MESH)

    @pl.loop(1, rows)
    def _(j):
        peer = (lax.rem(row + j, rows), col)
        pl.semaphore_signal(barrier, inc=1, device_id=peer, device_id_type=MESH)

    pl.semaphore_wait(barrier, rows + cols - 2)

    def far_first(j):
        return half + (j // 2) * (1 - 2 * (j % 2))

    def a_range(part, c):
        return pl.ds(part * xa + c * ca, ca)

    def b_range(part, c):
        return pl.ds(pl.multiple_of(part * yb + c * cb, SUBLANES), cb)

    def send_y(p, source):
        @pl.loop(0, ychunks)
        def _(c):
            pltpu.make_async_copy(
                source.at[p, a_range(col, c)], ybuf.at[p, c, col], yf_recv.at[p, c]
            ).start()

            @pl.loop(1, cols)
            def _(j):
                to = lax.rem(col + far_first(j), cols)
                pltpu.make_async_remote_copy(
                    source.at[p, a_range(to, c)],
                    ybuf.at[p, c, col],
                    yf_send.at[p],
                    yf_recv.at[p, c],
                    device_id=(row, to),
                    device_id_type=MESH,
                ).start()

    def return_y(p, c, target):
        pltpu.make_async_copy(
            ybuf.at[p, c, col], target.at[p, a_range(col, c)], yb_recv.at[p]
        ).start()

        kept = (p == last) & (c >= ychunks - tail)

        @pl.loop(1, cols)
        def _(j):
            to = lax.rem(col + far_first(j), cols)

            @pl.when(jnp.logical_not(kept & (j == 1)))
            def _():
                pltpu.make_async_remote_copy(
                    ybuf.at[p, c, to],
                    target.at[p, a_range(col, c)],
                    yb_send.at[p],
                    yb_recv.at[p],
                    device_id=(row, to),
                    device_id_type=MESH,
                ).start()

        @pl.when(kept)
        def _():
            pltpu.make_async_copy(
                ybuf.at[p, c, lax.rem(col + half, cols)],
                rest.at[pl.ds((c - (ychunks - tail)) * ca, ca)],
                rest_sem,
            ).start()

    def send_x(p, source):
        @pl.loop(0, xchunks)
        def _(c):
            pltpu.make_async_copy(
                source.at[p, :, b_range(row, c)], xbuf.at[p, c, row], xf_recv.at[p, c]
            ).start()

            @pl.loop(1, rows)
            def _(j):
                to = lax.rem(row + j, rows)
                pltpu.make_async_remote_copy(
                    source.at[p, :, b_range(to, c)],
                    xbuf.at[p, c, row],
                    xf_send.at[p],
                    xf_recv.at[p, c],
                    device_id=(to, col),
                    device_id_type=MESH,
                ).start()

    def return_x(p, c, target):
        pltpu.make_async_copy(
            xbuf.at[p, c, row], target.at[p, :, b_range(row, c)], xb_recv.at[p]
        ).start()

        @pl.loop(1, rows)
        def _(j):
            to = lax.rem(row + j, rows)
            pltpu.make_async_remote_copy(
                xbuf.at[p, c, to],
                target.at[p, :, b_range(row, c)],
                xb_send.at[p],
                xb_recv.at[p],
                device_id=(to, col),
                device_id_type=MESH,
            ).start()

    def prepare():
        for load in loads:
            load.wait()
        for raw, pair in ((raw_x, pair_x), (raw_y, pair_y)):
            pair[0], pair[1] = split(raw[...])
        turned = raw_z[...].T
        for p in range(params):
            pair_z[p, 0], pair_z[p, 1] = split(turned * raw_s[pl.ds(p, 1), :])

    def filter_y_depth(p, c):
        wait_bytes(ybuf.at[p, c], yf_recv.at[p, c])

        @pl.loop(0, ca)
        def _(a):
            plane = ybuf[p, c, :, a].reshape(cols * yloc, depth)
            column = dot3(split(plane), (pair_z[p, 0], pair_z[p, 1]))
            value = dot3((pair_y[0], pair_y[1]), split(column))
            ybuf[p, c, :, a] = value.reshape(cols, yloc, depth)

    def filter_x_rows(p, c):
        wait_bytes(xbuf.at[p, c], xf_recv.at[p, c])
        for b in range(cb):
            plane = xbuf[p, c, :, :, b, :].reshape(rows * xloc, depth)
            value = dot3((pair_x[0], pair_x[1]), split(plane))
            xbuf[p, c, :, :, b, :] = value.reshape(rows, xloc, depth)

    @pl.loop(0, params)
    def _(q):
        x_param = lax.rem(q + 1, params)

        @pl.when(q == 0)
        def _():
            send_y(0, field)
            send_x(1, field)
            prepare()

        @pl.when(q > 0)
        def _():
            wait_bytes(home.at[q], xb_recv.at[q])
            send_y(q, home)

            @pl.when(q < params - 1)
            def _():
                send_x(q + 1, field)

            @pl.when(q == params - 1)
            def _():
                wait_bytes(home.at[0], yb_recv.at[0])
                send_x(0, home)

        @pl.loop(0, max(xchunks, ychunks))
        def _(c):
            @pl.when(c < xchunks)
            def _():
                filter_x_rows(x_param, c)

                @pl.when(x_param > 0)
                def _():
                    return_x(x_param, c, home)

                @pl.when(x_param == 0)
                def _():
                    return_x(0, c, out)

            @pl.when(c < ychunks)
            def _():
                filter_y_depth(q, c)

                @pl.when(q == 0)
                def _():
                    return_y(0, c, home)

                @pl.when(q > 0)
                def _():
                    return_y(q, c, out)

    wait_bytes(out.at[0], xb_recv.at[0])

    @pl.loop(0, params)
    def _(p):
        wait_bytes(home.at[p, pl.ds(0, xloc - xa)], yf_send.at[p])

        @pl.when(p < last)
        def _():
            wait_bytes(home.at[p, pl.ds(0, xloc - xa)], yb_send.at[p])

            @pl.when(p > 0)
            def _():
                wait_bytes(out.at[p], yb_recv.at[p])

        @pl.when(p == last)
        def _():
            sent = xloc - tail * ca
            wait_bytes(out.at[p, pl.ds(0, sent)], yb_recv.at[p])
            wait_bytes(home.at[p, pl.ds(0, sent - xa)], yb_send.at[p])
            wait_bytes(rest, rest_sem)

        for sem in (xf_send, xb_send):
            wait_bytes(home.at[p, :, pl.ds(0, yloc - yb)], sem.at[p])


def place_kernel(given, out, slots, reads, writes):
    count, planes = slots.shape[:2]
    per = given.shape[1] // planes

    def part(ref, n):
        return ref.at[n // per, pl.ds(n % per * planes, planes)]

    def read(n):
        return pltpu.make_async_copy(part(given, n), slots.at[n], reads.at[n])

    def write(n):
        return pltpu.make_async_copy(slots.at[n], part(out, n), writes.at[n])

    for n in range(count):
        read(n).start()
    for n in range(count):
        read(n).wait()
        write(n).start()
    for n in range(count):
        write(n).wait()


def place(field):
    params, xloc, yloc, depth = field.shape
    planes = max(n for n in range(1, PLACE_PLANES + 1) if xloc % n == 0)
    count = params * xloc // planes
    return pl.pallas_call(
        place_kernel,
        in_specs=[pl.BlockSpec(memory_space=pl.ANY)],
        out_specs=pl.BlockSpec(memory_space=pl.ANY),
        out_shape=jax.ShapeDtypeStruct(field.shape, jnp.float32),
        scratch_shapes=[
            pltpu.VMEM((count, planes, yloc, depth), jnp.float32),
            pltpu.SemaphoreType.DMA((count,)),
            pltpu.SemaphoreType.DMA((count,)),
        ],
        cost_estimate=pl.CostEstimate(
            flops=512 * field.size, bytes_accessed=8 * field.size, transcendentals=0
        ),
        compiler_params=pltpu.CompilerParams(vmem_limit_bytes=VMEM_LIMIT - SPARE),
    )(field)


def insert_kernel(cols, landed, _, out, sem):
    params, xloc = out.shape[:2]
    planes, xa = landed.shape[0], xloc // cols
    source = lax.rem(lax.axis_index("col") + cols // 2, cols)
    target = out.at[params - 1, pl.ds((source + 1) * xa - planes, planes)]
    move = pltpu.make_async_copy(landed, target, sem)
    move.start()
    move.wait()


def insert(field, landed, cols):
    return pl.pallas_call(
        functools.partial(insert_kernel, cols),
        in_specs=[pl.BlockSpec(memory_space=pltpu.VMEM), pl.BlockSpec(memory_space=pl.ANY)],
        out_specs=pl.BlockSpec(memory_space=pl.ANY),
        out_shape=jax.ShapeDtypeStruct(field.shape, jnp.float32),
        input_output_aliases={1: 0},
        scratch_shapes=[pltpu.SemaphoreType.DMA],
        cost_estimate=pl.CostEstimate(
            flops=landed.size, bytes_accessed=8 * landed.size, transcendentals=0
        ),
        compiler_params=pltpu.CompilerParams(vmem_limit_bytes=SPARE),
    )(landed, field)


def kernel_shards(model_gradient, filter_x, filter_y, filter_z, depth_scale):
    rows, cols = lax.axis_size("row"), lax.axis_size("col")
    params, xloc, yloc, depth = model_gradient.shape
    nx, ny = filter_x.shape[0], filter_y.shape[0]
    ychunks = y_chunks(xloc // cols)
    ca = xloc // cols // ychunks
    tail = max(1, ychunks // 2)
    cb = SUBLANES
    xchunks = yloc // rows // cb
    whole = pl.BlockSpec(memory_space=pl.ANY)
    full = jax.ShapeDtypeStruct(model_gradient.shape, jnp.float32)
    dma = pltpu.SemaphoreType.DMA
    flops = 6 * model_gradient.size * (nx + ny + depth)
    held = jax.ShapeDtypeStruct((tail * ca, yloc, depth), jnp.float32)
    out, _, rest = pl.pallas_call(
        functools.partial(smooth_kernel, rows, cols, tail),
        in_specs=[whole] * 5,
        out_specs=[whole] * 3,
        out_shape=[full, full, held],
        scratch_shapes=[
            pltpu.VMEM((params, ychunks, cols, ca, yloc, depth), jnp.float32),
            pltpu.VMEM((params, xchunks, rows, xloc, cb, depth), jnp.float32),
            pltpu.VMEM(filter_x.shape, jnp.float32),
            pltpu.VMEM(filter_y.shape, jnp.float32),
            pltpu.VMEM(filter_z.shape, jnp.float32),
            pltpu.VMEM(depth_scale.shape, jnp.float32),
            pltpu.VMEM((2,) + filter_x.shape, jnp.bfloat16),
            pltpu.VMEM((2,) + filter_y.shape, jnp.bfloat16),
            pltpu.VMEM((params, 2) + filter_z.shape, jnp.bfloat16),
            dma((4,)),
            dma,
            dma((params, ychunks)),
            dma((params,)),
            dma((params, xchunks)),
            dma((params,)),
            dma((params,)),
            dma((params,)),
            dma((params,)),
            dma((params,)),
        ],
        cost_estimate=pl.CostEstimate(
            flops=flops, bytes_accessed=32 * model_gradient.size, transcendentals=0
        ),
        compiler_params=pltpu.CompilerParams(
            collective_id=0, has_side_effects=True, vmem_limit_bytes=VMEM_LIMIT
        ),
    )(model_gradient, filter_x, filter_y, filter_z, depth_scale)
    swap = [(s, (s + cols // 2) % cols) for s in range(cols)]
    landed = lax.ppermute(rest, "col", swap)
    return insert(place(out), landed, cols)


def y_chunks(planes):
    return 4 if planes % 4 == 0 else 1


def fits(shape, rows, cols):
    params, xloc, yloc, depth = shape
    aligned = cols % 2 == 0 and xloc % cols == 0 and depth % LANES == 0
    aligned = aligned and yloc % (rows * SUBLANES) == 0
    staged = 2 * 4 * params * xloc * yloc * depth
    return aligned and params > 1 and staged <= STAGING_LIMIT


def plane_filter(incoming, filter_x, filter_y, rows, cols):
    xloc, yloc = incoming.shape[0], incoming.shape[1]
    matrix_x = filter_x.reshape(rows, xloc, rows, xloc)
    matrix_y = filter_y.reshape(cols, yloc, cols, yloc)
    partial_value = jnp.einsum(
        "ABRa,abRSz->ABbSz", matrix_x, incoming, precision=ACCURACY
    )
    return jnp.einsum(
        "CDSb,ABbSz->ACBDz", matrix_y, partial_value, precision=ACCURACY
    )


def plain_shards(model_gradient, filter_x, filter_y, filter_z, depth_scale):
    rows, cols = lax.axis_size("row"), lax.axis_size("col")
    params, xloc, yloc, depth = model_gradient.shape
    parts = rows * cols
    block = depth // parts
    arrived = []
    for index in range(params):
        scaled_filter = depth_scale[index][:, None] * filter_z
        column = jnp.einsum(
            "kz,abz->abk", scaled_filter, model_gradient[index], precision=ACCURACY
        )
        outgoing = column.reshape(xloc, yloc, parts, block)
        arrived.append(
            lax.all_to_all(outgoing, AXES, split_axis=2, concat_axis=2, tiled=True)
        )
    results = []
    for index in range(params):
        incoming = arrived[index].reshape(xloc, yloc, rows, cols, block)
        planes = plane_filter(incoming, filter_x, filter_y, rows, cols)
        planes = planes.reshape(parts, xloc, yloc, block)
        back = lax.all_to_all(planes, AXES, split_axis=0, concat_axis=3, tiled=True)
        results.append(back.reshape(xloc, yloc, depth))
    return jnp.stack(results)


def shards(model_gradient, filter_x, filter_y, filter_z, depth_scale):
    rows, cols = lax.axis_size("row"), lax.axis_size("col")
    chosen = kernel_shards if fits(model_gradient.shape, rows, cols) else plain_shards
    return chosen(model_gradient, filter_x, filter_y, filter_z, depth_scale)


def solution(mesh):
    return jax.shard_map(
        shards,
        mesh=mesh,
        in_specs=(P(None, "row", "col", None), P(), P(), P(), P()),
        out_specs=P(None, "row", "col", None),
        check_vma=False,
    )
```
